32 devices in a mesh: pipe: 8 (over z, y), tensor: 4 (over x, core).
Axes of the slice: x: 2, y: 2, z: 4, core: 2. Of those that a mesh axis runs over, the one named last changes fastest.
Arguments:
- memory: bfloat16 [2, 512, 4096], P(None, 'pipe', 'tensor'), may hold values from -6 to 6
- states: bfloat16 [8, 2, 256, 4096], P('pipe', None, None, 'tensor'), may hold values from -6 to 6
- norm_gain: float32 [8, 4096], P('pipe'), may hold values from 0.25 to 1.75
- w_query: bfloat16 [8, 4096, 4096], P('pipe', None, 'tensor'), may hold values from -0.09375 to 0.09375
- w_keyvalue: bfloat16 [8, 4096, 2, 4096], P('pipe', None, None, 'tensor'), may hold values from -0.09375 to 0.09375
- w_output: bfloat16 [8, 4096, 4096], P('pipe', 'tensor'), may hold values from -0.125 to 0.125
Outputs:
- updated: bfloat16 [8, 2, 256, 4096], P('pipe', None, None, 'tensor')
The draws below stay inside these ranges and needn't reach their ends.
All inputs are finite; a program needn't handle non-finite values.
Results may differ from the reference program's by a relative error of at most 0.006.
Values may be sent and summed in bfloat16 or wider, within the bound.
A program may use at most 128 MiB of HBM per device.

```python
import jax
import jax.numpy as jnp
from jax import lax

D = 4096
HEADS = 64
HEAD_DIM = 64
INNER = 4096
SEQS = 2
ENC_LEN = 512
DEC_LEN = 256
SECTIONS = 8


def with_spikes(entries, stream_key, source, target, parts, factor):
    owner, partner = [(jnp.arange(entries.shape[dim]) // (entries.shape[dim] // parts)).reshape([-1 if axis == dim else 1 for axis in range(entries.ndim)]) for dim in (source, target)]
    chosen = jax.random.permutation(stream_key, parts)[partner]
    strong = (owner == chosen) | (owner == (partner + parts // 2) % parts)
    return jnp.where(strong, factor * entries, entries)


def levels(own_key, extent, shards, low, largest):
    level, own = 1.0, jax.random.fold_in(own_key, 6)
    for dim, parts in shards:
        steps = jnp.exp(jax.random.uniform(jax.random.fold_in(own, dim), (parts,), jnp.float32, low / len(shards), largest / len(shards)))
        level = level * jnp.repeat(steps, extent[dim] // parts).reshape([-1 if axis == dim else 1 for axis in range(len(extent))])
    return level


def scatter_about(rng, extent, scale, reach, split=(), held_as=jnp.bfloat16):
    result = jax.random.normal(rng, extent, jnp.float32) * scale
    if len(split) > 0:
        result = levels(rng, extent, split, -0.22, 0.18) * result
    return jnp.clip(result, min=-reach, max=reach).astype(held_as)


def noise_with(own_key, shape, spread, reach, split, heavy, dtype=jnp.bfloat16):
    values = spread * jax.random.normal(own_key, shape, jnp.float32)
    if split:
        values = values * levels(own_key, shape, split, -0.22, 0.18)
    return jnp.clip(with_spikes(values, jax.random.fold_in(own_key, 3), *heavy), -reach, reach).astype(dtype)


def setup_inputs(seed: int = 0) -> dict:
    key_of = jax.random.split(jax.random.key(seed), 7)
    return {
        "memory": scatter_about(key_of[0], (SEQS, ENC_LEN, D), 1.0, 6.0, ((1, 8), (2, 4))),
        "states": scatter_about(key_of[1], (SECTIONS, SEQS, DEC_LEN, D), 1.0, 6.0, ((0, 8), (3, 4))),
        "norm_gain": jnp.clip(1.0 + 0.15 * jax.random.normal(key_of[2], (SECTIONS, D), jnp.float32), 0.25, 1.75),
        "w_query": scatter_about(key_of[3], (SECTIONS, D, INNER), D ** -0.5, 0.09375, ((0, 8), (2, 4))),
        "w_keyvalue": scatter_about(key_of[4], (SECTIONS, D, 2, INNER), D ** -0.5, 0.09375, ((0, 8), (3, 4))),
        "w_output": noise_with(key_of[5], (SECTIONS, INNER, D), INNER ** -0.5, 0.125, ((0, 8), (1, 4)), (1, 2, 4, 2.0)),
    }


def one_section(memory, section_states, gain, wq, wkv, wo):
    xf = section_states.astype(jnp.float32)
    scale = lax.rsqrt(lax.optimization_barrier(jnp.mean(xf * xf, axis=-1, keepdims=True)) + 1e-06)
    normed = (xf * scale * gain).astype(jnp.bfloat16)
    seqs = normed.shape[0]
    inner = HEADS * HEAD_DIM
    wkv_flat = wkv.reshape(wkv.shape[0], 2 * inner)
    query = jnp.einsum('btd,de->bte', normed.astype(jnp.float32), wq.astype(jnp.float32)).astype(jnp.bfloat16)
    keyvalue = jnp.einsum('bpd,de->bpe', memory.astype(jnp.float32), wkv_flat.astype(jnp.float32)).astype(jnp.bfloat16)
    keys = keyvalue[:, :, :inner].reshape(seqs, ENC_LEN, HEADS, HEAD_DIM)
    values = keyvalue[:, :, inner:].reshape(seqs, ENC_LEN, HEADS, HEAD_DIM)
    qh = query.reshape(seqs, DEC_LEN, HEADS, HEAD_DIM)
    scores = jnp.einsum('bqhd,bkhd->bhqk', qh.astype(jnp.float32), keys.astype(jnp.float32)) / jnp.sqrt(jnp.float32(HEAD_DIM))
    probs = jax.nn.softmax(scores, axis=-1).astype(jnp.bfloat16)
    context = jnp.einsum('bhqk,bkhd->bqhd', probs.astype(jnp.float32), values.astype(jnp.float32)).astype(jnp.bfloat16)
    context = context.reshape(seqs, DEC_LEN, inner)
    branch = jnp.einsum('bte,ed->btd', context.astype(jnp.float32), wo.astype(jnp.float32))
    return (xf + branch).astype(jnp.bfloat16)

def reference(memory, states, norm_gain, w_query, w_keyvalue, w_output):

    def run(packed):
        section_states, gain, wq, wkv, wo = packed
        return one_section(memory, section_states, gain, wq, wkv, wo)
    return lax.map(run, (states, norm_gain, w_query, w_keyvalue, w_output))
```

```python
import functools

import jax
import jax.numpy as jnp
from jax import lax
from jax.experimental import pallas as pl
from jax.experimental.pallas import tpu as pltpu
from jax.sharding import PartitionSpec as P

HEAD_DIM = 64
CORES = 2
LOW = 2
TILE = 256
MAX_COPIES = 100
MESH = pl.DeviceIdType.MESH
F32 = jnp.float32
BF16 = jnp.bfloat16


def copies_per_sequence(n_pipe, n_tensor):
    xs, highs = n_tensor // CORES, n_pipe // LOW
    return 4 * n_pipe * xs + (xs - 1) * highs


def kernel(
    n_pipe, n_tensor,
    mem_hbm, st_hbm, gain_ref, wq_hbm, wkv_hbm, wo_hbm, out_ref,
    mem, st, wq, wkv, wo, q, kv, ctx, pd, rd, px, rx, part,
    load_sem, send_sem, recv_ici, recv_d2d, st_ici, st_d2d, pd_sem, px_sem,
):
    xs, highs = n_tensor // CORES, n_pipe // LOW
    seqs, enc, depth = mem.shape
    rows = st.shape[1]
    pos = enc // n_pipe
    feat = depth // n_tensor
    inner = wq.shape[1]
    pipe = lax.axis_index("pipe")
    tensor = lax.axis_index("tensor")
    hi, lo = pipe // LOW, pipe % LOW
    x, core = tensor // CORES, tensor % CORES
    other_lo, other_core = 1 - lo, 1 - core

    def turn(a, k, n):
        return lax.rem(a + k, n)

    def device(h, l, xx, c):
        return (h * LOW + l, xx * CORES + c)

    x_peers = [device(hi, lo, turn(x, j, xs), core) for j in range(1, xs)]
    hi_peers = [device(turn(hi, k, highs), lo, x, core) for k in range(1, highs)]
    lo_peer = device(hi, other_lo, x, core)
    sibling = device(hi, lo, x, other_core)

    def block(s, p, xx, c):
        r = pl.multiple_of(p * pos, pos)
        f = pl.multiple_of((xx * CORES + c) * feat, feat)
        return mem.at[s, pl.ds(r, pos), pl.ds(f, feat)]

    def st_block(s, xx, c):
        return st.at[s, :, pl.ds(pl.multiple_of((xx * CORES + c) * feat, feat), feat)]

    sends = []
    counter = [0]

    def new_sems(n=1):
        first = counter[0]
        counter[0] += n
        return first

    def remote(src, dst, sem, recv, dev):
        return pltpu.make_async_remote_copy(
            src_ref=src, dst_ref=dst, send_sem=send_sem.at[sem], recv_sem=recv,
            device_id=dev, device_id_type=MESH,
        )

    def send(src, dst, recv, dev):
        copy = remote(src, dst, new_sems(), recv, dev)
        copy.start()
        sends.append(copy)
        return copy

    st_sends = [[], []]

    def send_states(s, ref, recv, dev):
        st_sends[s].append(send(ref, ref, recv, dev))
        sends.pop()

    def send_block(s, p, xx, dev, recv):
        ref = block(s, p, xx, core)
        send(ref, ref, recv.at[s, p * xs + xx], dev)

    def wait_block(s, p, xx):
        ref = block(s, p, xx, core)
        remote(ref, ref, 0, recv_ici.at[s, p * xs + xx], sibling).wait_recv()

    loads = [
        pltpu.make_async_copy(mem_hbm.at[0], block(0, pipe, x, core), load_sem.at[0]),
        pltpu.make_async_copy(st_hbm.at[0], st_block(0, x, core), load_sem.at[1]),
        pltpu.make_async_copy(mem_hbm.at[1], block(1, pipe, x, core), load_sem.at[2]),
        pltpu.make_async_copy(st_hbm.at[1], st_block(1, x, core), load_sem.at[3]),
    ]
    weights = [
        pltpu.make_async_copy(wkv_hbm, wkv, load_sem.at[4]),
        pltpu.make_async_copy(wq_hbm, wq, load_sem.at[5]),
        pltpu.make_async_copy(wo_hbm, wo, load_sem.at[6]),
    ]
    for copy in loads:
        copy.start()
    barrier = pltpu.get_barrier_semaphore()
    peers = x_peers + hi_peers + [lo_peer, sibling]
    for peer in peers:
        pl.semaphore_signal(barrier, inc=1, device_id=peer, device_id_type=MESH)
    pl.semaphore_wait(barrier, len(peers))

    def first_sends(s):
        loads[2 * s].wait()
        for dev in x_peers:
            send_block(s, pipe, x, dev, recv_ici)
        send_block(s, pipe, x, lo_peer, recv_ici)
        for dev in hi_peers:
            send_block(s, pipe, x, dev, recv_ici)
        send_block(s, pipe, x, sibling, recv_d2d)

    def state_sends(s):
        loads[2 * s + 1].wait()
        ref = st_block(s, x, core)
        for dev in x_peers:
            send_states(s, ref, st_ici.at[s, x], dev)
        send_states(s, ref, st_d2d.at[s, x], sibling)

    def forward_x(s):
        for j in range(1, xs):
            xx = turn(x, j, xs)
            wait_block(s, pipe, xx)
            send_block(s, pipe, xx, lo_peer, recv_ici)
            for dev in hi_peers:
                send_block(s, pipe, xx, dev, recv_ici)
            send_block(s, pipe, xx, sibling, recv_d2d)

    n_high = (highs - 1) * xs

    def high_copies(s, i, base):
        k, j = 1 + i // xs, i % xs
        p, xx = turn(hi, k, highs) * LOW + lo, turn(x, j, xs)
        ref = block(s, p, xx, core)
        slot = p * xs + xx
        arrived = remote(ref, ref, 0, recv_ici.at[s, slot], sibling)
        return (
            arrived,
            remote(ref, ref, base + 2 * i, recv_ici.at[s, slot], lo_peer),
            remote(ref, ref, base + 2 * i + 1, recv_d2d.at[s, slot], sibling),
        )

    def forward_high(s, i, base):
        arrived, over_low, over = high_copies(s, i, base)
        arrived.wait_recv()
        over_low.start()
        over.start()

    high_base = [new_sems(2 * n_high), new_sems(2 * n_high)]

    def forward_low(s):
        for k in range(highs):
            for j in range(xs):
                p, xx = turn(hi, k, highs) * LOW + other_lo, turn(x, j, xs)
                wait_block(s, p, xx)
                send_block(s, p, xx, sibling, recv_d2d)

    def forward_states(s):
        for j in range(1, xs):
            xx = turn(x, j, xs)
            ref = st_block(s, xx, core)
            remote(ref, ref, 0, st_ici.at[s, xx], sibling).wait_recv()
            send_states(s, ref, st_d2d.at[s, xx], sibling)

    def finish_states(s):
        for xx in range(xs):
            ref = st_block(s, xx, other_core)
            remote(ref, ref, 0, st_d2d.at[s, xx], sibling).wait_recv()

    def finish_memory(s):
        for p in range(n_pipe):
            for xx in range(xs):
                ref = block(s, p, xx, other_core)
                remote(ref, ref, 0, recv_d2d.at[s, p * xs + xx], sibling).wait_recv()

    def query(s):
        for copy in st_sends[s]:
            copy.wait_send()
        part[s] = st[s, :, pl.ds(pl.multiple_of(tensor * feat, feat), feat)].astype(F32)

        @pl.loop(0, rows // 16)
        def _(i):
            some = pl.ds(pl.multiple_of(i * 16, 16), 16)
            xf = st[s, some, :].astype(F32)
            mean = jnp.sum(xf * xf, axis=-1, keepdims=True) * (1.0 / depth)
            scale = lax.rsqrt(mean + 1e-06)
            st[s, some, :] = (xf * scale * gain_ref[...]).astype(BF16)

        if s == 0:
            weights[1].wait()

        @pl.loop(0, inner // TILE)
        def _(i):
            cols = pl.ds(pl.multiple_of(i * TILE, TILE), TILE)
            full = jnp.dot(st[s], wq[:, cols], preferred_element_type=F32)
            q[s, :, cols] = full.astype(BF16) * jnp.array(HEAD_DIM ** -0.5, BF16)

    def kv_tile(s, i):
        cols = pl.ds(pl.multiple_of(i * TILE, TILE), TILE)
        full = jnp.dot(mem[s], wkv[:, cols], preferred_element_type=F32)
        kv[:, cols] = full.astype(BF16)

    def attention(s):
        lane = lax.broadcasted_iota(jnp.int32, (1, 2 * HEAD_DIM), 1)
        first = lane < HEAD_DIM

        @pl.loop(0, inner // (2 * HEAD_DIM))
        def _(i):
            cols = pl.ds(pl.multiple_of(i * 2 * HEAD_DIM, 2 * HEAD_DIM), 2 * HEAD_DIM)
            vcols = pl.ds(pl.multiple_of(inner + i * 2 * HEAD_DIM, 2 * HEAD_DIM), 2 * HEAD_DIM)
            qp, kp, vp = q[s, :, cols], kv[:, cols], kv[:, vcols]
            outs = []
            for mine in (first, jnp.logical_not(first)):
                qh = jnp.where(mine, qp, jnp.zeros_like(qp))
                vh = jnp.where(mine, vp, jnp.ones_like(vp))
                scores = lax.dot_general(
                    qh, kp, (((1,), (1,)), ((), ())), preferred_element_type=F32
                )
                top = jnp.max(scores, axis=-1, keepdims=True)
                probs = jnp.exp(scores - top).astype(BF16)
                outs.append(jnp.dot(probs, vh, preferred_element_type=F32))
            total = jnp.where(first, outs[0], outs[1])
            sums = pltpu.roll(jnp.where(first, outs[1], outs[0]), HEAD_DIM, 1)
            ctx[:, cols] = (total / sums).astype(BF16)

    width = min(TILE, feat)

    def product(t, i):
        cols = pl.ds(pl.multiple_of(t * feat + i * width, width), width)
        return jnp.dot(ctx[...], wo[:, cols], preferred_element_type=F32)

    def tile(i):
        return pl.ds(pl.multiple_of(i * width, width), width)

    def output(s):
        if s == 0:
            weights[2].wait()
        steps = feat // width
        order = [turn(x, j, xs) for j in range(1, xs)] + [x]
        for j, xx in enumerate(order):
            @pl.loop(0, steps)
            def _(i):
                pd[s, j, :, tile(i)] = product(xx * CORES + other_core, i).astype(BF16)

            send(pd.at[s, j], rd.at[s, j], pd_sem.at[s, j], sibling)
            if j < xs - 1:
                @pl.loop(0, steps)
                def _(i):
                    px[s, j, :, tile(i)] = product(xx * CORES + core, i).astype(BF16)

                remote(pd.at[s, j], rd.at[s, j], 0, pd_sem.at[s, j], sibling).wait_recv()
                px[s, j] = (px[s, j].astype(F32) + rd[s, j].astype(F32)).astype(BF16)
                send(px.at[s, j], rx.at[s, j], px_sem.at[s, j], x_peers[j])

    def result(s):
        j = xs - 1
        remote(pd.at[s, j], rd.at[s, j], 0, pd_sem.at[s, j], sibling).wait_recv()

        @pl.loop(0, feat // width)
        def _(i):
            c = tile(i)
            part[s, :, c] += product(tensor, i) + rd[s, j, :, c].astype(F32)

    def finish(s):
        for j in range(xs - 1):
            remote(px.at[s, j], rx.at[s, j], 0, px_sem.at[s, j], sibling).wait_recv()

        @pl.loop(0, feat // width)
        def _(i):
            c = tile(i)
            total = part[s, :, c]
            for j in range(xs - 1):
                total += rx[s, j, :, c].astype(F32)
            out_ref[s, :, c] = total.astype(BF16)

    for s in range(seqs):
        first_sends(s)
        state_sends(s)
        if s == 0:
            for copy in weights:
                copy.start()
    forward_x(0)
    half = n_high // 2
    for i in range(half):
        forward_high(0, i, high_base[0])
    forward_x(1)
    for i in range(half, n_high):
        forward_high(0, i, high_base[0])
    forward_states(0)
    finish_states(0)
    query(0)
    forward_low(0)
    weights[0].wait()
    finish_memory(0)
    tiles = 2 * inner // TILE

    @pl.loop(0, tiles)
    def _(i):
        @pl.when(i < n_high)
        def _():
            forward_high(1, i, high_base[1])

        kv_tile(0, i)

    for i in range(tiles, n_high):
        forward_high(1, i, high_base[1])
    attention(0)
    output(0)
    result(0)
    forward_states(1)
    finish_states(1)
    query(1)
    forward_low(1)
    finish_memory(1)

    @pl.loop(0, tiles)
    def _(i):
        kv_tile(1, i)

    attention(1)
    output(1)
    result(1)
    finish(0)
    finish(1)
    for copy in sends:
        copy.wait_send()
    for s in range(seqs):
        for i in range(n_high):
            arrived, over_low, over = high_copies(s, i, high_base[s])
            over_low.wait_send()
            over.wait_send()


def fused(n_pipe, n_tensor, memory, states, norm_gain, w_query, w_keyvalue, w_output):
    seqs, pos, feat = memory.shape
    rows = states.shape[2]
    depth, inner = feat * n_tensor, w_query.shape[2]
    enc = pos * n_pipe
    xs, highs = n_tensor // CORES, n_pipe // LOW
    weight_kv = w_keyvalue[0].reshape(depth, 2 * inner)
    blocks = n_pipe * xs
    per_seq = ((xs - 1) + (highs - 1) + 2 + (xs - 1) * (highs + 1) + 2 * (highs - 1) * xs
               + highs * xs + 2 * xs + 2 * xs)
    any_space = pl.BlockSpec(memory_space=pl.ANY)
    in_vmem = pl.BlockSpec(memory_space=pltpu.VMEM)
    dma = pltpu.SemaphoreType.DMA
    out = pl.pallas_call(
        functools.partial(kernel, n_pipe, n_tensor),
        out_shape=jax.ShapeDtypeStruct((seqs, rows, feat), BF16),
        in_specs=[any_space, any_space, in_vmem, any_space, any_space, any_space],
        out_specs=in_vmem,
        scratch_shapes=[
            pltpu.VMEM((seqs, enc, depth), BF16),
            pltpu.VMEM((seqs, rows, depth), BF16),
            pltpu.VMEM((depth, inner), BF16),
            pltpu.VMEM((depth, 2 * inner), BF16),
            pltpu.VMEM((inner, depth), BF16),
            pltpu.VMEM((seqs, rows, inner), BF16),
            pltpu.VMEM((enc, 2 * inner), BF16),
            pltpu.VMEM((rows, inner), BF16),
            pltpu.VMEM((seqs, xs, rows, feat), BF16),
            pltpu.VMEM((seqs, xs, rows, feat), BF16),
            pltpu.VMEM((seqs, xs - 1, rows, feat), BF16),
            pltpu.VMEM((seqs, xs - 1, rows, feat), BF16),
            pltpu.VMEM((seqs, rows, feat), F32),
            dma((7,)),
            dma((seqs * per_seq,)),
            dma((seqs, blocks)),
            dma((seqs, blocks)),
            dma((seqs, xs)),
            dma((seqs, xs)),
            dma((seqs, xs)),
            dma((seqs, xs - 1)),
        ],
        compiler_params=pltpu.CompilerParams(
            collective_id=0, has_side_effects=True, vmem_limit_bytes=66_000_000
        ),
    )(memory, states[0], norm_gain, w_query[0], weight_kv, w_output[0])
    return out[None]


def per_device(memory, states, norm_gain, w_query, w_keyvalue, w_output):
    whole_states = lax.all_gather(states[0], "tensor", axis=2, tiled=True)
    xf = whole_states.astype(jnp.float32)
    scale = lax.rsqrt(jnp.mean(xf * xf, axis=-1, keepdims=True) + 1e-06)
    normed = (xf * scale * norm_gain[0]).astype(jnp.bfloat16)
    weight_q = w_query[0]
    local_inner = weight_q.shape[1]
    weight_kv = w_keyvalue[0].reshape(w_keyvalue.shape[1], 2 * local_inner)
    weight_o = w_output[0]
    seqs = normed.shape[0]
    dec_rows = normed.shape[1]
    local_heads = local_inner // HEAD_DIM
    query = jnp.einsum("btd,de->bte", normed, weight_q, preferred_element_type=jnp.float32).astype(
        jnp.bfloat16
    )
    gathered = lax.all_gather(memory, "pipe", axis=1, tiled=True)
    gathered = lax.all_gather(gathered, "tensor", axis=2, tiled=True)
    keyvalue = jnp.einsum(
        "bpd,de->bpe", gathered, weight_kv, preferred_element_type=jnp.float32
    ).astype(jnp.bfloat16)
    enc_rows = keyvalue.shape[1]
    keys = keyvalue[:, :, :local_inner].reshape(seqs, enc_rows, local_heads, HEAD_DIM)
    values = keyvalue[:, :, local_inner:].reshape(seqs, enc_rows, local_heads, HEAD_DIM)
    heads_q = query.reshape(seqs, dec_rows, local_heads, HEAD_DIM)
    scores = jnp.einsum(
        "bqhd,bkhd->bhqk", heads_q, keys, preferred_element_type=jnp.float32
    ) / jnp.sqrt(jnp.float32(HEAD_DIM))
    probs = jax.nn.softmax(scores, axis=-1).astype(jnp.bfloat16)
    context = jnp.einsum(
        "bhqk,bkhd->bqhd", probs, values, preferred_element_type=jnp.float32
    ).astype(jnp.bfloat16)
    context = context.reshape(seqs, dec_rows, local_inner)
    partial_terms = jnp.einsum("bte,ed->btd", context, weight_o, preferred_element_type=jnp.float32)
    branch = lax.psum_scatter(partial_terms, "tensor", scatter_dimension=2, tiled=True)
    result = (states[0].astype(jnp.float32) + branch).astype(jnp.bfloat16)
    return result[None]


def solution(mesh):
    in_specs = (
        P(None, "pipe", "tensor"),
        P("pipe", None, None, "tensor"),
        P("pipe", None),
        P("pipe", None, "tensor"),
        P("pipe", None, None, "tensor"),
        P("pipe", "tensor", None),
    )
    out_specs = P("pipe", None, None, "tensor")
    n_pipe, n_tensor = mesh.shape["pipe"], mesh.shape["tensor"]
    even = n_pipe % LOW == 0 and n_tensor % CORES == 0 and n_pipe > LOW and n_tensor > CORES
    body = per_device
    if even and copies_per_sequence(n_pipe, n_tensor) <= MAX_COPIES:
        body = functools.partial(fused, n_pipe, n_tensor)
    return jax.shard_map(
        body, mesh=mesh, in_specs=in_specs, out_specs=out_specs, check_vma=False
    )
```

```python
import functools

import jax
import jax.numpy as jnp
from jax import lax
from jax.experimental import pallas as pl
from jax.experimental.pallas import tpu as pltpu
from jax.sharding import PartitionSpec as P

HEAD_DIM = 64
CORES = 2
LOW = 2
TILE = 256
MAX_COPIES = 100
LANES = 128
SUB = 16
CHUNK = 256
MESH = pl.DeviceIdType.MESH
F32 = jnp.float32
BF16 = jnp.bfloat16


def copies_per_sequence(n_pipe, n_tensor):
    xs, highs = n_tensor // CORES, n_pipe // LOW
    return 4 * n_pipe * xs + (xs - 1) * highs


def kernel(
    n_pipe, n_tensor,
    mem_hbm, st_hbm, gain_ref, wq_hbm, wkv_hbm, wo_hbm, out_ref,
    mem, st, wq, wkv, wo, q, kv, ctx, pd, rd, px, rx, part, staged,
    load_sem, stage_sem, send_sem, recv_ici, recv_d2d, st_ici, st_d2d, pd_sem, px_sem,
):
    xs, highs = n_tensor // CORES, n_pipe // LOW
    seqs, enc, depth = mem.shape
    rows = st.shape[1]
    pos = enc // n_pipe
    feat = depth // n_tensor
    inner = wq.shape[1]
    pipe = lax.axis_index("pipe")
    tensor = lax.axis_index("tensor")
    hi, lo = pipe // LOW, pipe % LOW
    x, core = tensor // CORES, tensor % CORES
    other_lo, other_core = 1 - lo, 1 - core

    def turn(a, k, n):
        return lax.rem(a + k, n)

    def device(h, l, xx, c):
        return (h * LOW + l, xx * CORES + c)

    x_peers = [device(hi, lo, turn(x, j, xs), core) for j in range(1, xs)]
    hi_peers = [device(turn(hi, k, highs), lo, x, core) for k in range(1, highs)]
    lo_peer = device(hi, other_lo, x, core)
    sibling = device(hi, lo, x, other_core)

    def block(s, p, xx, c):
        r = pl.multiple_of(p * pos, pos)
        f = pl.multiple_of((xx * CORES + c) * feat, feat)
        return mem.at[s, pl.ds(r, pos), pl.ds(f, feat)]

    def st_block(s, xx, c):
        return st.at[s, :, pl.ds(pl.multiple_of((xx * CORES + c) * feat, feat), feat)]

    sends = []
    counter = [0]

    def new_sems(n=1):
        first = counter[0]
        counter[0] += n
        return first

    def remote(src, dst, sem, recv, dev):
        return pltpu.make_async_remote_copy(
            src_ref=src, dst_ref=dst, send_sem=send_sem.at[sem], recv_sem=recv,
            device_id=dev, device_id_type=MESH,
        )

    def send(src, dst, recv, dev):
        copy = remote(src, dst, new_sems(), recv, dev)
        copy.start()
        sends.append(copy)
        return copy

    st_sends = [[], []]

    def send_states(s, ref, recv, dev):
        st_sends[s].append(send(ref, ref, recv, dev))
        sends.pop()

    def send_block(s, p, xx, dev, recv):
        ref = block(s, p, xx, core)
        send(ref, ref, recv.at[s, p * xs + xx], dev)

    def wait_block(s, p, xx):
        ref = block(s, p, xx, core)
        remote(ref, ref, 0, recv_ici.at[s, p * xs + xx], sibling).wait_recv()

    loads = [
        pltpu.make_async_copy(mem_hbm.at[0], block(0, pipe, x, core), load_sem.at[0]),
        pltpu.make_async_copy(st_hbm.at[0], st_block(0, x, core), load_sem.at[1]),
        pltpu.make_async_copy(mem_hbm.at[1], block(1, pipe, x, core), load_sem.at[2]),
        pltpu.make_async_copy(st_hbm.at[1], st_block(1, x, core), load_sem.at[3]),
    ]
    weights = [
        pltpu.make_async_copy(wq_hbm, wq, load_sem.at[4]),
        pltpu.make_async_copy(wo_hbm, wo, load_sem.at[5]),
    ]
    for copy in loads:
        copy.start()
    barrier = pltpu.get_barrier_semaphore()
    peers = x_peers + hi_peers + [lo_peer, sibling]
    for peer in peers:
        pl.semaphore_signal(barrier, inc=1, device_id=peer, device_id_type=MESH)
    pl.semaphore_wait(barrier, len(peers))

    def first_sends(s):
        loads[2 * s].wait()
        for dev in x_peers:
            send_block(s, pipe, x, dev, recv_ici)
        send_block(s, pipe, x, lo_peer, recv_ici)
        for dev in hi_peers:
            send_block(s, pipe, x, dev, recv_ici)
        send_block(s, pipe, x, sibling, recv_d2d)

    def state_sends(s):
        loads[2 * s + 1].wait()
        ref = st_block(s, x, core)
        for dev in x_peers:
            send_states(s, ref, st_ici.at[s, x], dev)
        send_states(s, ref, st_d2d.at[s, x], sibling)

    def forward_x(s):
        for j in range(1, xs):
            xx = turn(x, j, xs)
            wait_block(s, pipe, xx)
            send_block(s, pipe, xx, lo_peer, recv_ici)
            for dev in hi_peers:
                send_block(s, pipe, xx, dev, recv_ici)
            send_block(s, pipe, xx, sibling, recv_d2d)

    n_high = (highs - 1) * xs

    def high_copies(s, i, base):
        k, j = 1 + i // xs, i % xs
        p, xx = turn(hi, k, highs) * LOW + lo, turn(x, j, xs)
        ref = block(s, p, xx, core)
        slot = p * xs + xx
        arrived = remote(ref, ref, 0, recv_ici.at[s, slot], sibling)
        return (
            arrived,
            remote(ref, ref, base + 2 * i, recv_ici.at[s, slot], lo_peer),
            remote(ref, ref, base + 2 * i + 1, recv_d2d.at[s, slot], sibling),
        )

    def forward_high(s, i, base):
        arrived, over_low, over = high_copies(s, i, base)
        arrived.wait_recv()
        over_low.start()
        over.start()

    high_base = [new_sems(2 * n_high), new_sems(2 * n_high)]

    def forward_low(s):
        for k in range(highs):
            for j in range(xs):
                p, xx = turn(hi, k, highs) * LOW + other_lo, turn(x, j, xs)
                wait_block(s, p, xx)
                send_block(s, p, xx, sibling, recv_d2d)

    def forward_states(s):
        for j in range(1, xs):
            xx = turn(x, j, xs)
            ref = st_block(s, xx, core)
            remote(ref, ref, 0, st_ici.at[s, xx], sibling).wait_recv()
            send_states(s, ref, st_d2d.at[s, xx], sibling)

    def finish_states(s):
        for xx in range(xs):
            ref = st_block(s, xx, other_core)
            remote(ref, ref, 0, st_d2d.at[s, xx], sibling).wait_recv()

    def finish_memory(s):
        for p in range(n_pipe):
            for xx in range(xs):
                ref = block(s, p, xx, other_core)
                remote(ref, ref, 0, recv_d2d.at[s, p * xs + xx], sibling).wait_recv()

    def query(s):
        for copy in st_sends[s]:
            copy.wait_send()
        part[s] = st[s, :, pl.ds(pl.multiple_of(tensor * feat, feat), feat)].astype(F32)

        @pl.loop(0, rows // 16)
        def _(i):
            some = pl.ds(pl.multiple_of(i * 16, 16), 16)
            xf = st[s, some, :].astype(F32)
            mean = jnp.sum(xf * xf, axis=-1, keepdims=True) * (1.0 / depth)
            scale = lax.rsqrt(mean + 1e-06)
            st[s, some, :] = (xf * scale * gain_ref[...]).astype(BF16)

        if s == 0:
            weights[0].wait()

        @pl.loop(0, inner // TILE)
        def _(i):
            cols = pl.ds(pl.multiple_of(i * TILE, TILE), TILE)
            full = jnp.dot(st[s], wq[:, cols], preferred_element_type=F32)
            q[s, :, cols] = full.astype(BF16) * jnp.array(HEAD_DIM ** -0.5, BF16)

    def kv_tile(s, i):
        cols = pl.ds(pl.multiple_of(i * TILE, TILE), TILE)
        full = jnp.dot(mem[s], wkv[:, cols], preferred_element_type=F32)
        kv[:, cols] = full.astype(BF16)

    def attention(s):
        lane = lax.broadcasted_iota(jnp.int32, (1, 2 * HEAD_DIM), 1)
        first = lane < HEAD_DIM

        @pl.loop(0, inner // (2 * HEAD_DIM))
        def _(i):
            cols = pl.ds(pl.multiple_of(i * 2 * HEAD_DIM, 2 * HEAD_DIM), 2 * HEAD_DIM)
            vcols = pl.ds(pl.multiple_of(inner + i * 2 * HEAD_DIM, 2 * HEAD_DIM), 2 * HEAD_DIM)
            qp, kp, vp = q[s, :, cols], kv[:, cols], kv[:, vcols]
            outs = []
            for mine in (first, jnp.logical_not(first)):
                qh = jnp.where(mine, qp, jnp.zeros_like(qp))
                vh = jnp.where(mine, vp, jnp.ones_like(vp))
                scores = lax.dot_general(
                    qh, kp, (((1,), (1,)), ((), ())), preferred_element_type=F32
                )
                top = jnp.max(scores, axis=-1, keepdims=True)
                probs = jnp.exp(scores - top).astype(BF16)
                outs.append(jnp.dot(probs, vh, preferred_element_type=F32))
            total = jnp.where(first, outs[0], outs[1])
            sums = pltpu.roll(jnp.where(first, outs[1], outs[0]), HEAD_DIM, 1)
            ctx[:, cols] = (total / sums).astype(BF16)

    width = min(TILE, feat)

    def product(t, i):
        cols = pl.ds(pl.multiple_of(t * feat + i * width, width), width)
        return jnp.dot(ctx[...], wo[:, cols], preferred_element_type=F32)

    def tile(i):
        return pl.ds(pl.multiple_of(i * width, width), width)

    def output(s):
        if s == 0:
            weights[1].wait()
        steps = feat // width
        order = [turn(x, j, xs) for j in range(1, xs)] + [x]
        for j, xx in enumerate(order):
            @pl.loop(0, steps)
            def _(i):
                pd[s, j, :, tile(i)] = product(xx * CORES + other_core, i).astype(BF16)

            send(pd.at[s, j], rd.at[s, j], pd_sem.at[s, j], sibling)
            if j < xs - 1:
                @pl.loop(0, steps)
                def _(i):
                    px[s, j, :, tile(i)] = product(xx * CORES + core, i).astype(BF16)

                remote(pd.at[s, j], rd.at[s, j], 0, pd_sem.at[s, j], sibling).wait_recv()
                px[s, j] = (px[s, j].astype(F32) + rd[s, j].astype(F32)).astype(BF16)
                send(px.at[s, j], rx.at[s, j], px_sem.at[s, j], x_peers[j])

    def result(s):
        j = xs - 1
        remote(pd.at[s, j], rd.at[s, j], 0, pd_sem.at[s, j], sibling).wait_recv()

        @pl.loop(0, feat // width)
        def _(i):
            c = tile(i)
            part[s, :, c] += product(tensor, i) + rd[s, j, :, c].astype(F32)

    def finish(s):
        for j in range(xs - 1):
            remote(px.at[s, j], rx.at[s, j], 0, px_sem.at[s, j], sibling).wait_recv()

        @pl.loop(0, feat // width)
        def _(i):
            c = tile(i)
            total = part[s, :, c]
            for j in range(xs - 1):
                total += rx[s, j, :, c].astype(F32)
            out_ref[s, :, c] = total.astype(BF16)

    groups = 2 * inner // LANES
    size = CHUNK * groups
    chunks = depth // CHUNK

    def stage(i, slot):
        src = wkv_hbm.at[pl.ds(pl.multiple_of(i * size, size), size), :]
        return pltpu.make_async_copy(src, staged.at[slot], stage_sem.at[slot])

    def spread(begin, end):
        span = SUB * groups
        a = lax.broadcasted_iota(jnp.int32, (span, span), 0)
        b = lax.broadcasted_iota(jnp.int32, (span, span), 1)
        swap = (b == lax.rem(a, SUB) * groups + a // SUB).astype(F32).astype(BF16)

        @pl.loop(begin, end)
        def _(i):
            slot = lax.rem(i, 2)
            stage(i, slot).wait()

            @pl.loop(0, CHUNK // (2 * SUB))
            def _(m):
                r = pl.multiple_of(m * 2 * span, 2 * span)
                both = jnp.concatenate(
                    [staged[slot, pl.ds(r, span), :], staged[slot, pl.ds(r + span, span), :]], axis=1
                )
                moved = jnp.dot(swap, both, preferred_element_type=F32).astype(BF16)
                d = pl.multiple_of(i * CHUNK + m * 2 * SUB, 2 * SUB)
                for g in range(groups):
                    col = (g % 2) * inner + (g // 2) * LANES
                    piece = moved[g * SUB:(g + 1) * SUB]
                    wkv[pl.ds(d, SUB), col:col + LANES] = piece[:, :LANES]
                    wkv[pl.ds(d + SUB, SUB), col:col + LANES] = piece[:, LANES:]

            @pl.when(i + 2 < chunks)
            def _():
                stage(i + 2, slot).start()

    for i in range(2):
        stage(i, i).start()
    for s in range(seqs):
        first_sends(s)
        state_sends(s)
        if s == 0:
            for copy in weights:
                copy.start()
    spread(0, chunks // 4)
    forward_x(0)
    spread(chunks // 4, chunks)
    half = n_high // 2
    for i in range(half):
        forward_high(0, i, high_base[0])
    forward_x(1)
    for i in range(half, n_high):
        forward_high(0, i, high_base[0])
    forward_states(0)
    finish_states(0)
    query(0)
    forward_low(0)
    forward_states(1)
    finish_states(1)
    query(1)
    finish_memory(0)
    tiles = 2 * inner // TILE

    @pl.loop(0, tiles)
    def _(i):
        @pl.when(i < n_high)
        def _():
            forward_high(1, i, high_base[1])

        kv_tile(0, i)

    for i in range(tiles, n_high):
        forward_high(1, i, high_base[1])
    attention(0)
    output(0)
    forward_low(1)
    result(0)
    finish_memory(1)

    @pl.loop(0, tiles)
    def _(i):
        kv_tile(1, i)

    attention(1)
    output(1)
    result(1)
    finish(0)
    finish(1)
    for copy in sends:
        copy.wait_send()
    for s in range(seqs):
        for i in range(n_high):
            arrived, over_low, over = high_copies(s, i, high_base[s])
            over_low.wait_send()
            over.wait_send()


def fused(n_pipe, n_tensor, memory, states, norm_gain, w_query, w_keyvalue, w_output):
    seqs, pos, feat = memory.shape
    rows = states.shape[2]
    depth, inner = feat * n_tensor, w_query.shape[2]
    enc = pos * n_pipe
    xs, highs = n_tensor // CORES, n_pipe // LOW
    groups = 2 * inner // LANES
    weight_kv = w_keyvalue[0].reshape(depth, 2, inner // LANES, LANES)
    weight_kv = weight_kv.transpose(0, 2, 1, 3).reshape(depth * groups, LANES)
    blocks = n_pipe * xs
    per_seq = ((xs - 1) + (highs - 1) + 2 + (xs - 1) * (highs + 1) + 2 * (highs - 1) * xs
               + highs * xs + 2 * xs + 2 * xs)
    any_space = pl.BlockSpec(memory_space=pl.ANY)
    in_vmem = pl.BlockSpec(memory_space=pltpu.VMEM)
    dma = pltpu.SemaphoreType.DMA
    out = pl.pallas_call(
        functools.partial(kernel, n_pipe, n_tensor),
        out_shape=jax.ShapeDtypeStruct((seqs, rows, feat), BF16),
        in_specs=[any_space, any_space, in_vmem, any_space, any_space, any_space],
        out_specs=in_vmem,
        scratch_shapes=[
            pltpu.VMEM((seqs, enc, depth), BF16),
            pltpu.VMEM((seqs, rows, depth), BF16),
            pltpu.VMEM((depth, inner), BF16),
            pltpu.VMEM((depth, 2 * inner), BF16),
            pltpu.VMEM((inner, depth), BF16),
            pltpu.VMEM((seqs, rows, inner), BF16),
            pltpu.VMEM((enc, 2 * inner), BF16),
            pltpu.VMEM((rows, inner), BF16),
            pltpu.VMEM((seqs, xs, rows, feat), BF16),
            pltpu.VMEM((seqs, xs, rows, feat), BF16),
            pltpu.VMEM((seqs, xs - 1, rows, feat), BF16),
            pltpu.VMEM((seqs, xs - 1, rows, feat), BF16),
            pltpu.VMEM((seqs, rows, feat), F32),
            pltpu.VMEM((2, CHUNK * groups, LANES), BF16),
            dma((6,)),
            dma((2,)),
            dma((seqs * per_seq,)),
            dma((seqs, blocks)),
            dma((seqs, blocks)),
            dma((seqs, xs)),
            dma((seqs, xs)),
            dma((seqs, xs)),
            dma((seqs, xs - 1)),
        ],
        compiler_params=pltpu.CompilerParams(
            collective_id=0, has_side_effects=True, vmem_limit_bytes=66_000_000
        ),
    )(memory, states[0], norm_gain, w_query[0], weight_kv, w_output[0])
    return out[None]


def per_device(memory, states, norm_gain, w_query, w_keyvalue, w_output):
    whole_states = lax.all_gather(states[0], "tensor", axis=2, tiled=True)
    xf = whole_states.astype(jnp.float32)
    scale = lax.rsqrt(jnp.mean(xf * xf, axis=-1, keepdims=True) + 1e-06)
    normed = (xf * scale * norm_gain[0]).astype(jnp.bfloat16)
    weight_q = w_query[0]
    local_inner = weight_q.shape[1]
    weight_kv = w_keyvalue[0].reshape(w_keyvalue.shape[1], 2 * local_inner)
    weight_o = w_output[0]
    seqs = normed.shape[0]
    dec_rows = normed.shape[1]
    local_heads = local_inner // HEAD_DIM
    query = jnp.einsum("btd,de->bte", normed, weight_q, preferred_element_type=jnp.float32).astype(
        jnp.bfloat16
    )
    gathered = lax.all_gather(memory, "pipe", axis=1, tiled=True)
    gathered = lax.all_gather(gathered, "tensor", axis=2, tiled=True)
    keyvalue = jnp.einsum(
        "bpd,de->bpe", gathered, weight_kv, preferred_element_type=jnp.float32
    ).astype(jnp.bfloat16)
    enc_rows = keyvalue.shape[1]
    keys = keyvalue[:, :, :local_inner].reshape(seqs, enc_rows, local_heads, HEAD_DIM)
    values = keyvalue[:, :, local_inner:].reshape(seqs, enc_rows, local_heads, HEAD_DIM)
    heads_q = query.reshape(seqs, dec_rows, local_heads, HEAD_DIM)
    scores = jnp.einsum(
        "bqhd,bkhd->bhqk", heads_q, keys, preferred_element_type=jnp.float32
    ) / jnp.sqrt(jnp.float32(HEAD_DIM))
    probs = jax.nn.softmax(scores, axis=-1).astype(jnp.bfloat16)
    context = jnp.einsum(
        "bhqk,bkhd->bqhd", probs, values, preferred_element_type=jnp.float32
    ).astype(jnp.bfloat16)
    context = context.reshape(seqs, dec_rows, local_inner)
    partial_terms = jnp.einsum("bte,ed->btd", context, weight_o, preferred_element_type=jnp.float32)
    branch = lax.psum_scatter(partial_terms, "tensor", scatter_dimension=2, tiled=True)
    result = (states[0].astype(jnp.float32) + branch).astype(jnp.bfloat16)
    return result[None]


def solution(mesh):
    in_specs = (
        P(None, "pipe", "tensor"),
        P("pipe", None, None, "tensor"),
        P("pipe", None),
        P("pipe", None, "tensor"),
        P("pipe", None, None, "tensor"),
        P("pipe", "tensor", None),
    )
    out_specs = P("pipe", None, None, "tensor")
    n_pipe, n_tensor = mesh.shape["pipe"], mesh.shape["tensor"]
    even = n_pipe % LOW == 0 and n_tensor % CORES == 0 and n_pipe > LOW and n_tensor > CORES
    body = per_device
    if even and copies_per_sequence(n_pipe, n_tensor) <= MAX_COPIES:
        body = functools.partial(fused, n_pipe, n_tensor)
    return jax.shard_map(
        body, mesh=mesh, in_specs=in_specs, out_specs=out_specs, check_vma=False
    )
```
